512 devices in a mesh: section: 32 (over x, y_hi, core), dp: 16 (over y_lo, z).
Axes of the slice: x: 4, y: 8 (y_hi: 4, y_lo: 2; y = y_hi * 2 + y_lo), z: 8, core: 2. Of those that a mesh axis runs over, the one named last changes fastest.
Arguments:
- out_pair: float32 [2048, 2048], P('dp'), may hold values from -6 to 6
- out_grad: bfloat16 [2048, 2048], P('dp'), may hold values from -6 to 6
- f_weight: bfloat16 [32, 1024, 1024], P('section', 'dp'), may hold values from -0.09375 to 0.09375
- g_weight: bfloat16 [32, 1024, 1024], P('section', 'dp'), may hold values from -0.09375 to 0.09375
- gains: float32 [32, 2, 1024], P('section'), may hold values from 0.1 to 1.9
Outputs:
- in_pair: float32 [32, 2048, 2048], P('section', 'dp')
- in_grad: bfloat16 [32, 2048, 2048], P('section', 'dp')
- f_grad: float32 [32, 1024, 1024], P('section', 'dp')
- g_grad: float32 [32, 1024, 1024], P('section', 'dp')
- gains_grad: float32 [32, 2, 1024], P('section')
The draws below stay inside these ranges and needn't reach their ends.
All inputs are finite; a program needn't handle non-finite values.
Results may differ from the reference program's by a relative error of at most 0.04.
Values may be sent and summed in bfloat16 or wider, within the bound.
No kernel may reach another device: no remote copies, remote signals or barrier semaphores. Data moves between devices by JAX's collectives and lax.ppermute only.
A program may use at most 64 MiB of HBM per device.

```python
import jax
import jax.numpy as jnp
from jax import lax

DH = 1024
TOK_DEV = 128
SECTIONS = 32
TOKENS = 2048
N_SECTION = 32
N_DP = 16


def steps_of(key, extent, shards, smallest, top_value):
    gain, own = 1.0, jax.random.fold_in(key, 6)
    for dim, parts in shards:
        steps = jnp.exp(jax.random.uniform(jax.random.fold_in(own, dim), (parts,), jnp.float32, smallest / len(shards), top_value / len(shards)))
        gain = gain * jnp.repeat(steps, extent[dim] // parts).reshape([-1 if axis == dim else 1 for axis in range(len(extent))])
    return gain


def centred(key, dims, width, reach, shards=(), kind=jnp.bfloat16):
    result = width * jax.random.normal(key, dims, jnp.float32)
    if shards:
        result = result * steps_of(key, dims, shards, -0.22, 0.18)
    return jnp.clip(result, -reach, reach).astype(kind)


def setup_inputs(seed: int = 0) -> dict:
    seeds = jax.random.split(jax.random.key(seed), 6)
    out_pair = centred(seeds[0], (TOKENS, 2 * DH), 1.0, 6.0, ((0, 16),), jnp.float32)
    out_grad = centred(seeds[1], (TOKENS, 2 * DH), 1.0, 6.0, ((0, 16),))
    f_weight = centred(seeds[2], (SECTIONS, DH, DH), (4 * DH) ** -0.5, 0.09375, ((0, 32), (1, 16)))
    g_weight = centred(seeds[3], (SECTIONS, DH, DH), (4 * DH) ** -0.5, 0.09375, ((0, 32), (1, 16)))
    gains = jnp.clip(1.0 + 0.18 * jax.random.normal(seeds[4], (SECTIONS, 2, DH), jnp.float32), 0.1, 1.9)
    return {"out_pair": out_pair, "out_grad": out_grad, "f_weight": f_weight, "g_weight": g_weight, "gains": gains}


offset = 0.25

def silu_parts(pre_values):
    sigmoid_value = jax.nn.sigmoid(pre_values)
    return (pre_values * sigmoid_value, sigmoid_value * (1.0 + pre_values * (1.0 - sigmoid_value)))

def normalize(values, gain_row):
    inv_scale = lax.rsqrt(lax.optimization_barrier(jnp.mean(values * values, axis=-1, keepdims=True)) + offset)
    return ((values * inv_scale * gain_row).astype(jnp.bfloat16), inv_scale)

def norm_back(values, inv_scale, gain_row, upstream):
    weighted = gain_row * upstream
    cubed = inv_scale * inv_scale * inv_scale
    return inv_scale * weighted - values * cubed * lax.optimization_barrier(jnp.mean(weighted * values, axis=-1, keepdims=True))

def coupling_back(upper_out, lower_out, upper_grad, lower_grad, w_first, w_second, gain_pair):
    normed_second, scale_second = normalize(upper_out, gain_pair[1])
    pre_second = jnp.dot(normed_second, w_second, preferred_element_type=jnp.float32)
    act_second, slope_second = silu_parts(pre_second)
    lower_in = lower_out - act_second
    normed_first, scale_first = normalize(lower_in, gain_pair[0])
    pre_first = jnp.dot(normed_first, w_first, preferred_element_type=jnp.float32)
    act_first, slope_first = silu_parts(pre_first)
    upper_in = upper_out - act_first
    delta_second = (lower_grad * slope_second).astype(jnp.bfloat16)
    back_second = jnp.dot(delta_second, w_second.T, preferred_element_type=jnp.float32)
    through = upper_grad + norm_back(upper_out, scale_second, gain_pair[1], back_second)
    delta_first = (through * slope_first).astype(jnp.bfloat16)
    back_first = jnp.dot(delta_first, w_first.T, preferred_element_type=jnp.float32)
    lower_total = lower_grad + norm_back(lower_in, scale_first, gain_pair[0], back_first)
    gain_terms = jnp.stack([lax.optimization_barrier(jnp.sum(back_first * lower_in * scale_first, axis=0)), lax.optimization_barrier(jnp.sum(back_second * upper_out * scale_second, axis=0))])
    return (upper_in, lower_in, through.astype(jnp.bfloat16), lower_total.astype(jnp.bfloat16), normed_first, delta_first, normed_second, delta_second, gain_terms)

def replica_sum(normed, delta):
    left_side = normed.reshape(N_DP, TOK_DEV, -1).astype(jnp.float32)
    right_side = delta.reshape(N_DP, TOK_DEV, -1).astype(jnp.float32)
    partial_sums = jnp.einsum('rtd,rte->rde', left_side, right_side)
    rounded = lax.optimization_barrier(partial_sums.astype(jnp.bfloat16))
    return lax.optimization_barrier(jnp.sum(rounded.astype(jnp.float32), axis=0))

def reference(out_pair, out_grad, f_weight, g_weight, gains):
    channels = out_pair.shape[1] // 2
    pair_now = out_pair
    grad_now = out_grad
    pairs, grads, first_sums, second_sums, gain_sums = ([], [], [], [], [])
    for layer_index in range(N_SECTION - 1, -1, -1):
        results = coupling_back(pair_now[:, :channels], pair_now[:, channels:], grad_now[:, :channels].astype(jnp.float32), grad_now[:, channels:].astype(jnp.float32), f_weight[layer_index], g_weight[layer_index], gains[layer_index])
        pair_now = jnp.concatenate([results[0], results[1]], axis=1)
        grad_now = jnp.concatenate([results[2], results[3]], axis=1)
        pairs.append(pair_now)
        grads.append(grad_now)
        first_sums.append(replica_sum(results[4], results[5]))
        second_sums.append(replica_sum(results[6], results[7]))
        gain_sums.append(results[8])
    return (jnp.stack(pairs[::-1]), jnp.stack(grads[::-1]), jnp.stack(first_sums[::-1]), jnp.stack(second_sums[::-1]), jnp.stack(gain_sums[::-1]))
```

```python
import functools

import jax
import jax.numpy as jnp
from jax import lax
from jax.experimental import pallas as pl
from jax.experimental.pallas import tpu as pltpu
from jax.sharding import Mesh
from jax.sharding import PartitionSpec as P

offset = 0.25
CH = 1024
LAYERS = 8
ROWS = 16
F32, BF16 = jnp.float32, jnp.bfloat16


def silu_parts(pre):
    s = jax.nn.sigmoid(pre)
    return pre * s, s * (1.0 + pre * (1.0 - s))


def normalize(values, gain_row):
    inv = lax.rsqrt(jnp.mean(values * values, axis=-1, keepdims=True) + offset)
    return (values * inv * gain_row).astype(BF16), inv


def norm_back(values, inv, gain_row, upstream):
    weighted = gain_row * upstream
    return inv * weighted - values * (inv * inv * inv) * jnp.mean(
        weighted * values, axis=-1, keepdims=True
    )


def times(a, w):
    return jnp.dot(a, w, preferred_element_type=F32)


def times_transposed(a, w):
    return lax.dot_general(a, w, (((1,), (1,)), ((), ())), preferred_element_type=F32)


def layer_back(y1, y2, gy1, gy2, w_f, w_g, gain_f, gain_g):
    norm_g, inv_g = normalize(y1, gain_g)
    act_g, slope_g = silu_parts(times(norm_g, w_g()))
    x2 = y2 - act_g
    delta_g = (gy2 * slope_g).astype(BF16)
    norm_f, inv_f = normalize(x2, gain_f)
    act_f, slope_f = silu_parts(times(norm_f, w_f()))
    x1 = y1 - act_f
    back_g = times_transposed(delta_g, w_g())
    gz = gy1 + norm_back(y1, inv_g, gain_g, back_g)
    delta_f = (gz * slope_f).astype(BF16)
    back_f = times_transposed(delta_f, w_f())
    gx2 = gy2 + norm_back(x2, inv_f, gain_f, back_f)
    return x1, x2, gz, gx2, norm_f, delta_f, norm_g, delta_g, back_f, back_g, inv_f, inv_g


def stage_kernel(info, state, gains, own, other, bnd_in, bnd, out, wbuf, bbuf, wsem, bsem):
    del bnd_in

    def fetch(j, slot):
        layer = LAYERS - 1 - j
        row = (layer // 2) * CH
        mine = lax.rem(layer, 2) == info[1]

        @pl.when(mine)
        def _():
            pltpu.make_async_copy(own.at[pl.ds(row, CH)], wbuf.at[slot], wsem.at[slot]).start()

        @pl.when(jnp.logical_not(mine))
        def _():
            pltpu.make_async_copy(other.at[pl.ds(row, CH)], wbuf.at[slot], wsem.at[slot]).start()

    @pl.when(info[0] == 1)
    def _():
        fetch(0, 0)

        def step(j, carry):
            y1, y2, gy1, gy2 = carry
            slot = lax.rem(j, 2)
            layer = LAYERS - 1 - j
            bbuf[layer, :, 0:CH] = y1.astype(BF16)
            bbuf[layer, :, CH : 2 * CH] = y2.astype(BF16)
            bbuf[layer, :, 2 * CH : 3 * CH] = gy1.astype(BF16)
            bbuf[layer, :, 3 * CH : 4 * CH] = gy2.astype(BF16)
            pltpu.make_async_copy(own.at[pl.ds(0, CH)], wbuf.at[slot], wsem.at[slot]).wait()

            @pl.when(j < LAYERS - 1)
            def _():
                fetch(j + 1, 1 - slot)

            r = layer_back(
                y1,
                y2,
                gy1,
                gy2,
                lambda: wbuf[slot, :, 0:CH],
                lambda: wbuf[slot, :, CH : 2 * CH],
                gains[layer, 0:1, :],
                gains[layer, 1:2, :],
            )
            pltpu.make_async_copy(bbuf.at[layer], bnd.at[layer], bsem.at[layer]).start()
            return (r[0], r[1], r[2].astype(BF16).astype(F32), r[3].astype(BF16).astype(F32))

        first = tuple(state[:, k * CH : (k + 1) * CH].astype(F32) for k in range(4))
        last = lax.fori_loop(0, LAYERS, step, first)
        for k in range(4):
            out[:, k * CH : (k + 1) * CH] = last[k].astype(BF16)
        for k in range(LAYERS):
            pltpu.make_async_copy(bbuf.at[k], bnd.at[k], bsem.at[k]).wait()


def run_stage(info, state, gains, own, other, bnd):
    vmem = pl.BlockSpec(memory_space=pltpu.VMEM)
    hbm = pl.BlockSpec(memory_space=pl.ANY)
    return pl.pallas_call(
        stage_kernel,
        out_shape=(
            jax.ShapeDtypeStruct((LAYERS, ROWS, 4 * CH), BF16),
            jax.ShapeDtypeStruct((ROWS, 4 * CH), BF16),
        ),
        in_specs=[pl.BlockSpec(memory_space=pltpu.SMEM), vmem, vmem, hbm, hbm, hbm],
        out_specs=(hbm, vmem),
        scratch_shapes=[
            pltpu.VMEM((2, CH, 2 * CH), BF16),
            pltpu.VMEM((LAYERS, ROWS, 4 * CH), BF16),
            pltpu.SemaphoreType.DMA((2,)),
            pltpu.SemaphoreType.DMA((LAYERS,)),
        ],
        input_output_aliases={5: 0},
        compiler_params=pltpu.CompilerParams(vmem_limit_bytes=28 * 2**20),
        cost_estimate=pl.CostEstimate(
            flops=8 * 8 * ROWS * CH * CH, bytes_accessed=32 * 2**20, transcendentals=0
        ),
        name="stage",
    )(info, state, gains, own, other, bnd)


def owner_kernel(info, b, gains, own, pair, grad, parts, gain_sums, wbuf, wsem):
    copy = pltpu.make_async_copy(own.at[pl.ds(info[0] * CH, CH)], wbuf, wsem)
    copy.start()
    copy.wait()
    y1, y2, gy1, gy2 = (b[:, k * CH : (k + 1) * CH].astype(F32) for k in range(4))
    r = layer_back(
        y1,
        y2,
        gy1,
        gy2,
        lambda: wbuf[:, 0:CH],
        lambda: wbuf[:, CH : 2 * CH],
        gains[0:1, :],
        gains[1:2, :],
    )
    x1, x2, gz, gx2, norm_f, delta_f, norm_g, delta_g, back_f, back_g, inv_f, inv_g = r
    pair[:, 0:CH] = x1
    pair[:, CH : 2 * CH] = x2
    grad[:, 0:CH] = gz.astype(BF16)
    grad[:, CH : 2 * CH] = gx2.astype(BF16)
    gain_sums[0:1, :] = jnp.sum(back_f * x2 * inv_f, axis=0, keepdims=True)
    gain_sums[1:2, :] = jnp.sum(back_g * y1 * inv_g, axis=0, keepdims=True)
    contract = (((0,), (0,)), ((), ()))
    for at, n, d in ((0, norm_f, delta_f), (CH, norm_g, delta_g)):
        for k in range(0, CH, 256):
            part = lax.dot_general(n[:, k : k + 256], d, contract, preferred_element_type=F32)
            parts[k : k + 256, at : at + CH] = part.astype(BF16)


def run_owner(info, b, gains, own):
    vmem = pl.BlockSpec(memory_space=pltpu.VMEM)
    rows = b.shape[0]
    return pl.pallas_call(
        owner_kernel,
        out_shape=(
            jax.ShapeDtypeStruct((rows, 2 * CH), F32),
            jax.ShapeDtypeStruct((rows, 2 * CH), BF16),
            jax.ShapeDtypeStruct((CH, 2 * CH), BF16),
            jax.ShapeDtypeStruct((2, CH), F32),
        ),
        in_specs=[pl.BlockSpec(memory_space=pltpu.SMEM), vmem, vmem, pl.BlockSpec(memory_space=pl.ANY)],
        out_specs=(vmem, vmem, vmem, vmem),
        scratch_shapes=[pltpu.VMEM((CH, 2 * CH), BF16), pltpu.SemaphoreType.DMA],
        compiler_params=pltpu.CompilerParams(vmem_limit_bytes=48 * 2**20),
        cost_estimate=pl.CostEstimate(
            flops=12 * rows * CH * CH, bytes_accessed=12 * 2**20, transcendentals=0
        ),
        name="owner",
    )(info, b, gains, own)


def shards(out_pair, out_grad, f_weight, g_weight, gains):
    x, yh, c = (lax.axis_index(a) for a in ("x", "yh", "c"))
    shard = jnp.concatenate([f_weight[0], g_weight[0]], axis=1)
    own = lax.all_gather(shard, ("yh", "yl", "z"), axis=0, tiled=True)
    other = lax.ppermute(own, "c", [(0, 1), (1, 0)])
    all_gains = lax.all_gather(gains[0], ("yh", "c"), axis=0, tiled=False)
    at = (yh * 2 + c) * ROWS
    state = jnp.concatenate(
        [
            lax.dynamic_slice_in_dim(out_pair, at, ROWS, 0).astype(BF16),
            lax.dynamic_slice_in_dim(out_grad, at, ROWS, 0),
        ],
        axis=1,
    )
    bnd = jnp.zeros((LAYERS, ROWS, 4 * CH), BF16)
    for stage in range(4):
        info = jnp.stack([(x == 3 - stage).astype(jnp.int32), c.astype(jnp.int32)])
        bnd, out = run_stage(info, state, all_gains, own, other, bnd)
        if stage < 3:
            state = lax.ppermute(out, "x", [(3 - stage, 2 - stage)])
    mine = lax.all_to_all(bnd, ("yh", "c"), split_axis=0, concat_axis=0, tiled=True)
    mine = mine.reshape(LAYERS * ROWS, 4 * CH)
    info = jnp.reshape(yh, (1,)).astype(jnp.int32)
    pair, grad, parts, gain_part = run_owner(info, mine, gains[0], own)
    sums = lax.psum_scatter(parts, ("yl", "z"), scatter_dimension=0, tiled=True).astype(F32)
    gain_total = lax.psum(gain_part, ("yl", "z"))
    return (pair[None], grad[None], sums[None, :, :CH], sums[None, :, CH:], gain_total[None])


def solution(mesh):
    devices = mesh.devices.reshape(4, 4, 2, 2, 8)
    fine = Mesh(devices, ("x", "yh", "c", "yl", "z"))
    section, dp = ("x", "yh", "c"), ("yl", "z")
    return jax.shard_map(
        shards,
        mesh=fine,
        in_specs=(P(dp, None), P(dp, None), P(section, dp, None), P(section, dp, None), P(section, None, None)),
        out_specs=(
            P(section, dp, None),
            P(section, dp, None),
            P(section, dp, None),
            P(section, dp, None),
            P(section, None, None),
        ),
        check_vma=False,
    )
```

```python
import functools

import jax
import jax.numpy as jnp
from jax import lax
from jax.experimental import pallas as pl
from jax.experimental.pallas import tpu as pltpu
from jax.sharding import Mesh
from jax.sharding import PartitionSpec as P

offset = 0.25
CH = 1024
LAYERS = 8
ROWS = 16
F32, BF16 = jnp.float32, jnp.bfloat16


def silu_parts(pre):
    s = jax.nn.sigmoid(pre)
    return pre * s, s * (1.0 + pre * (1.0 - s))


def normalize(values, gain_row):
    inv = lax.rsqrt(jnp.mean(values * values, axis=-1, keepdims=True) + offset)
    return (values * inv * gain_row).astype(BF16), inv


def norm_back(values, inv, gain_row, upstream):
    weighted = gain_row * upstream
    return inv * weighted - values * (inv * inv * inv) * jnp.mean(
        weighted * values, axis=-1, keepdims=True
    )


def times(a, w):
    return jnp.dot(a, w, preferred_element_type=F32)


def times_transposed(a, w):
    return lax.dot_general(a, w, (((1,), (1,)), ((), ())), preferred_element_type=F32)


def pair_back(y1, y2, w_f, w_g, gain_f, gain_g):
    norm_g, inv_g = normalize(y1, gain_g)
    act_g, slope_g = silu_parts(times(norm_g, w_g))
    x2 = y2 - act_g
    norm_f, inv_f = normalize(x2, gain_f)
    act_f, slope_f = silu_parts(times(norm_f, w_f))
    return y1 - act_f, x2, slope_f, slope_g, inv_f, inv_g, norm_f, norm_g


def grad_back(gy1, gy2, y1, x2, slope_f, slope_g, inv_f, inv_g, w_f, w_g, gain_f, gain_g):
    delta_g = (gy2 * slope_g).astype(BF16)
    back_g = times_transposed(delta_g, w_g)
    gz = gy1 + norm_back(y1, inv_g, gain_g, back_g)
    delta_f = (gz * slope_f).astype(BF16)
    back_f = times_transposed(delta_f, w_f)
    gx2 = gy2 + norm_back(x2, inv_f, gain_f, back_f)
    return gz, gx2, delta_f, delta_g, back_f, back_g


def stage_kernel(info, state, gains, own, other, bnd_in, bnd, out, wbuf, bbuf, wsem, bsem):
    del bnd_in

    def fetch(j, slot):
        layer = LAYERS - 1 - j
        row = (layer // 2) * CH
        mine = lax.rem(layer, 2) == info[1]

        @pl.when(mine)
        def _():
            pltpu.make_async_copy(own.at[pl.ds(row, CH)], wbuf.at[slot], wsem.at[slot]).start()

        @pl.when(jnp.logical_not(mine))
        def _():
            pltpu.make_async_copy(other.at[pl.ds(row, CH)], wbuf.at[slot], wsem.at[slot]).start()

    def gain_rows(j):
        layer = LAYERS - 1 - j
        far = lax.rem(info[2] - layer // 2 + 4, 4)
        part = lax.rem(layer, 2)
        return gains[far, part, 0:1, :], gains[far, part, 1:2, :]

    def weights(j):
        slot = lax.rem(j, 3)
        return wbuf[slot, :, 0:CH], wbuf[slot, :, CH : 2 * CH]

    def pairs(j, y1, y2):
        slot = lax.rem(j, 3)
        layer = LAYERS - 1 - j
        bbuf[layer, :, 0:CH] = y1.astype(BF16)
        bbuf[layer, :, CH : 2 * CH] = y2.astype(BF16)
        pltpu.make_async_copy(own.at[pl.ds(0, CH)], wbuf.at[slot], wsem.at[slot]).wait()
        r = pair_back(y1, y2, *weights(j), *gain_rows(j))
        return r[0], r[1], (y1,) + r[1:6]

    def grads(j, gy1, gy2, kept):
        layer = LAYERS - 1 - j
        bbuf[layer, :, 2 * CH : 3 * CH] = gy1.astype(BF16)
        bbuf[layer, :, 3 * CH : 4 * CH] = gy2.astype(BF16)
        r = grad_back(gy1, gy2, *kept, *weights(j), *gain_rows(j))
        return r[0].astype(BF16).astype(F32), r[1].astype(BF16).astype(F32)

    @pl.when(info[0] == 1)
    def _():
        fetch(0, 0)
        fetch(1, 1)
        y1, y2, gy1, gy2 = (state[:, k * CH : (k + 1) * CH].astype(F32) for k in range(4))
        x1, x2, kept = pairs(0, y1, y2)

        def step(j, carry):
            y1, y2, gy1, gy2, kept = carry

            @pl.when(j < LAYERS - 1)
            def _():
                fetch(j + 1, lax.rem(j + 1, 3))

            x1, x2, fresh = pairs(j, y1, y2)
            gz, gx2 = grads(j - 1, gy1, gy2, kept)
            return x1, x2, gz, gx2, fresh

        x1, x2, gy1, gy2, kept = lax.fori_loop(1, LAYERS, step, (x1, x2, gy1, gy2, kept))
        gz, gx2 = grads(LAYERS - 1, gy1, gy2, kept)
        for k, v in enumerate((x1, x2, gz, gx2)):
            out[:, k * CH : (k + 1) * CH] = v.astype(BF16)
        copy = pltpu.make_async_copy(bbuf, bnd, bsem)
        copy.start()
        copy.wait()


def run_stage(info, state, gains, own, other, bnd):
    vmem = pl.BlockSpec(memory_space=pltpu.VMEM)
    hbm = pl.BlockSpec(memory_space=pltpu.HBM)
    return pl.pallas_call(
        stage_kernel,
        out_shape=(
            jax.ShapeDtypeStruct((LAYERS, ROWS, 4 * CH), BF16),
            jax.ShapeDtypeStruct((ROWS, 4 * CH), BF16),
        ),
        in_specs=[pl.BlockSpec(memory_space=pltpu.SMEM), vmem, vmem, hbm, hbm, hbm],
        out_specs=(hbm, vmem),
        scratch_shapes=[
            pltpu.VMEM((3, CH, 2 * CH), BF16),
            pltpu.VMEM((LAYERS, ROWS, 4 * CH), BF16),
            pltpu.SemaphoreType.DMA((3,)),
            pltpu.SemaphoreType.DMA,
        ],
        input_output_aliases={5: 0},
        compiler_params=pltpu.CompilerParams(vmem_limit_bytes=56 * 2**20),
        cost_estimate=pl.CostEstimate(
            flops=8 * 8 * ROWS * CH * CH, bytes_accessed=32 * 2**20, transcendentals=0
        ),
        name="stage",
    )(info, state, gains, own, other, bnd)


def owner_kernel(info, b, gains, own, pair, grad, parts, gain_sums, wbuf, wsem):
    copy = pltpu.make_async_copy(own.at[pl.ds(info[0] * CH, CH)], wbuf, wsem)
    copy.start()
    copy.wait()
    y1, y2, gy1, gy2 = (b[:, k * CH : (k + 1) * CH].astype(F32) for k in range(4))
    w_f, w_g = wbuf[:, 0:CH], wbuf[:, CH : 2 * CH]
    gain_f, gain_g = gains[0:1, :], gains[1:2, :]
    x1, x2, slope_f, slope_g, inv_f, inv_g, norm_f, norm_g = pair_back(y1, y2, w_f, w_g, gain_f, gain_g)
    gz, gx2, delta_f, delta_g, back_f, back_g = grad_back(
        gy1, gy2, y1, x2, slope_f, slope_g, inv_f, inv_g, w_f, w_g, gain_f, gain_g
    )
    pair[:, 0:CH] = x1
    pair[:, CH : 2 * CH] = x2
    grad[:, 0:CH] = gz.astype(BF16)
    grad[:, CH : 2 * CH] = gx2.astype(BF16)
    gain_sums[0:1, :] = jnp.sum(back_f * x2 * inv_f, axis=0, keepdims=True)
    gain_sums[1:2, :] = jnp.sum(back_g * y1 * inv_g, axis=0, keepdims=True)
    contract = (((0,), (0,)), ((), ()))
    for at, n, d in ((0, norm_f, delta_f), (CH, norm_g, delta_g)):
        for k in range(0, CH, 256):
            part = lax.dot_general(n[:, k : k + 256], d, contract, preferred_element_type=F32)
            parts[k : k + 256, at : at + CH] = part.astype(BF16)


def run_owner(info, b, gains, own):
    vmem = pl.BlockSpec(memory_space=pltpu.VMEM)
    rows = b.shape[0]
    return pl.pallas_call(
        owner_kernel,
        out_shape=(
            jax.ShapeDtypeStruct((rows, 2 * CH), F32),
            jax.ShapeDtypeStruct((rows, 2 * CH), BF16),
            jax.ShapeDtypeStruct((CH, 2 * CH), BF16),
            jax.ShapeDtypeStruct((2, CH), F32),
        ),
        in_specs=[pl.BlockSpec(memory_space=pltpu.SMEM), vmem, vmem, pl.BlockSpec(memory_space=pltpu.HBM)],
        out_specs=(vmem, vmem, vmem, vmem),
        scratch_shapes=[pltpu.VMEM((CH, 2 * CH), BF16), pltpu.SemaphoreType.DMA],
        compiler_params=pltpu.CompilerParams(vmem_limit_bytes=52 * 2**20),
        cost_estimate=pl.CostEstimate(
            flops=12 * rows * CH * CH, bytes_accessed=12 * 2**20, transcendentals=0
        ),
        name="owner",
    )(info, b, gains, own)


def shards(out_pair, out_grad, f_weight, g_weight, gains):
    x, yh, c = (lax.axis_index(a) for a in ("x", "yh", "c"))
    shard = jnp.concatenate([f_weight[0], g_weight[0]], axis=1)
    own = lax.all_gather(shard, ("yh", "yl", "z"), axis=0, tiled=True)
    other = lax.ppermute(own, "c", [(0, 1), (1, 0)])
    swapped = lax.ppermute(gains[0], "c", [(0, 1), (1, 0)])
    chip_gains = jnp.where(c == 0, jnp.stack([gains[0], swapped]), jnp.stack([swapped, gains[0]]))
    far_gains = [
        lax.ppermute(chip_gains, "yh", [(i, (i + by) % 4) for i in range(4)]) for by in (1, 2, 3)
    ]
    all_gains = jnp.stack([chip_gains] + far_gains)
    at = (yh * 2 + c) * ROWS
    state = jnp.concatenate(
        [
            lax.dynamic_slice_in_dim(out_pair, at, ROWS, 0).astype(BF16),
            lax.dynamic_slice_in_dim(out_grad, at, ROWS, 0),
        ],
        axis=1,
    )
    bnd = jnp.zeros((LAYERS, ROWS, 4 * CH), BF16)
    for stage in range(4):
        info = jnp.stack([(x == 3 - stage).astype(jnp.int32), c.astype(jnp.int32), yh.astype(jnp.int32)])
        bnd, out = run_stage(info, state, all_gains, own, other, bnd)
        if stage < 3:
            state = lax.ppermute(out, "x", [(3 - stage, 2 - stage)])
    mine = lax.all_to_all(bnd, ("yh", "c"), split_axis=0, concat_axis=0, tiled=True)
    mine = mine.reshape(LAYERS * ROWS, 4 * CH)
    info = jnp.reshape(yh, (1,)).astype(jnp.int32)
    pair, grad, parts, gain_part = run_owner(info, mine, gains[0], own)
    sums = lax.psum_scatter(parts, ("yl", "z"), scatter_dimension=0, tiled=True).astype(F32)
    gain_total = lax.psum(gain_part, ("yl", "z"))
    return (pair[None], grad[None], sums[None, :, :CH], sums[None, :, CH:], gain_total[None])


def solution(mesh):
    devices = mesh.devices.reshape(4, 4, 2, 2, 8)
    fine = Mesh(devices, ("x", "yh", "c", "yl", "z"))
    section, dp = ("x", "yh", "c"), ("yl", "z")
    return jax.shard_map(
        shards,
        mesh=fine,
        in_specs=(P(dp, None), P(dp, None), P(section, dp, None), P(section, dp, None), P(section, None, None)),
        out_specs=(
            P(section, dp, None),
            P(section, dp, None),
            P(section, dp, None),
            P(section, dp, None),
            P(section, None, None),
        ),
        check_vma=False,
    )
```

```python
import jax
import jax.numpy as jnp
from jax import lax
from jax.experimental import pallas as pl
from jax.experimental.pallas import tpu as pltpu
from jax.sharding import Mesh
from jax.sharding import PartitionSpec as P


offset = 0.25
CH = 1024
LAYERS = 8
ROWS = 16
F32, BF16 = jnp.float32, jnp.bfloat16


def silu_parts(pre):
    s = jax.nn.sigmoid(pre)
    return pre * s, s * (1.0 + pre * (1.0 - s))


def normalize(values, gain_row):
    inv = lax.rsqrt(jnp.mean(values * values, axis=-1, keepdims=True) + offset)
    return (values * inv * gain_row).astype(BF16), inv


def norm_back(values, inv, gain_row, upstream):
    weighted = gain_row * upstream
    return inv * weighted - values * (inv * inv * inv) * jnp.mean(
        weighted * values, axis=-1, keepdims=True
    )


def times(a, w):
    return jnp.dot(a, w, preferred_element_type=F32)


def times_transposed(a, w):
    return lax.dot_general(a, w, (((1,), (1,)), ((), ())), preferred_element_type=F32)


def pair_back(y1, y2, w_f, w_g, gain_f, gain_g):
    norm_g, inv_g = normalize(y1, gain_g)
    act_g, slope_g = silu_parts(times(norm_g, w_g()))
    x2 = y2 - act_g
    norm_f, inv_f = normalize(x2, gain_f)
    act_f, slope_f = silu_parts(times(norm_f, w_f()))
    return y1 - act_f, x2, slope_f, slope_g, inv_f, inv_g, norm_f, norm_g


def grad_back(gy1, gy2, y1, x2, slope_f, slope_g, inv_f, inv_g, w_f, w_g, gain_f, gain_g):
    delta_g = (gy2 * slope_g).astype(BF16)
    back_g = times_transposed(delta_g, w_g)
    gz = gy1 + norm_back(y1, inv_g, gain_g, back_g)
    delta_f = (gz * slope_f).astype(BF16)
    back_f = times_transposed(delta_f, w_f)
    gx2 = gy2 + norm_back(x2, inv_f, gain_f, back_f)
    return gz, gx2, delta_f, delta_g, back_f, back_g


N_REFS = 10


def block_copies(layer, f_ref, g_refs, y_me, z_me, w_f, w_g, sem_f, sem_g):
    for yl in range(2):
        far = lax.rem(y_me - (layer // 2) * 2 - yl + 8, 8)
        for r in range(8):

            @pl.when(far == r)
            def _(r=r, yl=yl):
                for p in range(8):
                    if r == 4:
                        src = g_refs[4 if p < 4 else 8].at[pl.ds((p % 4) * 64, 64)]
                    else:
                        src = g_refs[r].at[pl.ds(p * 64, 64)]
                    rows = pl.ds((yl * 8 + lax.rem(z_me - p + 8, 8)) * 64, 64)
                    pltpu.make_async_copy(src, w_g.at[rows], sem_g).start()

    pltpu.make_async_copy(f_ref.at[pl.ds((layer // 2) * CH, CH)], w_f, sem_f).start()


def stage_kernel(info, state, gains, *refs):
    own, other = refs[:N_REFS], refs[N_REFS : 2 * N_REFS]
    bnd, out, w_f, w_g, bbuf, sem_f, sem_g, bsem = refs[2 * N_REFS + 1 :]

    def fetch(j):
        slot = lax.rem(j, 3)
        layer = LAYERS - 1 - j
        mine = lax.rem(layer, 2) == info[1]
        for want, blocks in ((mine, own), (jnp.logical_not(mine), other)):

            @pl.when(want)
            def _(blocks=blocks):
                block_copies(
                    layer,
                    blocks[0],
                    blocks[1:],
                    info[2],
                    info[3],
                    w_f.at[slot],
                    w_g.at[slot],
                    sem_f.at[slot],
                    sem_g.at[slot],
                )

    def gain_rows(j):
        layer = LAYERS - 1 - j
        far = lax.rem(info[2] // 2 - layer // 2 + 4, 4)
        part = lax.rem(layer, 2)
        return gains[far, part, 0:1, :], gains[far, part, 1:2, :]

    def weights(j):
        slot = lax.rem(j, 3)
        return w_f[slot], w_g[slot]

    def pairs(j, y1, y2):
        slot = lax.rem(j, 3)
        layer = LAYERS - 1 - j
        bbuf[layer, :, 0:CH] = y1.astype(BF16)
        bbuf[layer, :, CH : 2 * CH] = y2.astype(BF16)

        def arrived(buf, sem):
            pltpu.make_async_copy(buf.at[slot], buf.at[slot], sem.at[slot]).wait()
            return buf[slot]

        r = pair_back(
            y1, y2, lambda: arrived(w_f, sem_f), lambda: arrived(w_g, sem_g), *gain_rows(j)
        )
        return r[0], r[1], (y1,) + r[1:6]

    def grads(j, gy1, gy2, kept):
        layer = LAYERS - 1 - j
        bbuf[layer, :, 2 * CH : 3 * CH] = gy1.astype(BF16)
        bbuf[layer, :, 3 * CH : 4 * CH] = gy2.astype(BF16)
        r = grad_back(gy1, gy2, *kept, *weights(j), *gain_rows(j))
        pltpu.make_async_copy(bbuf.at[layer], bnd.at[layer], bsem).start()
        return r[0].astype(BF16).astype(F32), r[1].astype(BF16).astype(F32)

    @pl.when(info[0] == 1)
    def _():
        def first_fetch(j, carry):
            fetch(j)
            return carry

        lax.fori_loop(0, 2, first_fetch, 0)
        y1, y2, gy1, gy2 = (state[:, k * CH : (k + 1) * CH].astype(F32) for k in range(4))
        x1, x2, kept = pairs(0, y1, y2)

        def step(j, carry):
            y1, y2, gy1, gy2, kept = carry

            @pl.when(j < LAYERS - 1)
            def _():
                fetch(j + 1)

            x1, x2, fresh = pairs(j, y1, y2)
            gz, gx2 = grads(j - 1, gy1, gy2, kept)
            return x1, x2, gz, gx2, fresh

        x1, x2, gy1, gy2, kept = lax.fori_loop(1, LAYERS, step, (x1, x2, gy1, gy2, kept))
        gz, gx2 = grads(LAYERS - 1, gy1, gy2, kept)
        for k, v in enumerate((x1, x2, gz, gx2)):
            out[:, k * CH : (k + 1) * CH] = v.astype(BF16)
        pltpu.make_async_copy(bbuf, bnd, bsem).wait()


def run_stage(info, state, gains, own, other, bnd):
    vmem = pl.BlockSpec(memory_space=pltpu.VMEM)
    hbm = pl.BlockSpec(memory_space=pltpu.HBM)
    return pl.pallas_call(
        stage_kernel,
        out_shape=(
            jax.ShapeDtypeStruct((LAYERS, ROWS, 4 * CH), BF16),
            jax.ShapeDtypeStruct((ROWS, 4 * CH), BF16),
        ),
        in_specs=[pl.BlockSpec(memory_space=pltpu.SMEM), vmem, vmem] + [hbm] * (2 * N_REFS + 1),
        out_specs=(hbm, vmem),
        scratch_shapes=[
            pltpu.VMEM((3, CH, CH), BF16),
            pltpu.VMEM((3, CH, CH), BF16),
            pltpu.VMEM((LAYERS, ROWS, 4 * CH), BF16),
            pltpu.SemaphoreType.DMA((3,)),
            pltpu.SemaphoreType.DMA((3,)),
            pltpu.SemaphoreType.DMA,
        ],
        input_output_aliases={3 + 2 * N_REFS: 0},
        compiler_params=pltpu.CompilerParams(vmem_limit_bytes=60 * 2**20),
        cost_estimate=pl.CostEstimate(
            flops=8 * 8 * ROWS * CH * CH, bytes_accessed=32 * 2**20, transcendentals=0
        ),
        name="stage",
    )(info, state, gains, *own, *other, bnd)


def owner_kernel(info, b, gains, *refs):
    own = refs[:N_REFS]
    pair, grad, parts, gain_sums, wbuf_f, wbuf_g, sem_f, sem_g = refs[N_REFS:]
    layer = (info[0] // 2) * 2
    block_copies(layer, own[0], own[1:], info[0], info[1], wbuf_f, wbuf_g, sem_f, sem_g)
    y1, y2, gy1, gy2 = (b[:, k * CH : (k + 1) * CH].astype(F32) for k in range(4))

    def arrived(buf, sem):
        pltpu.make_async_copy(buf, buf, sem).wait()
        return buf[...]

    gain_f, gain_g = gains[0:1, :], gains[1:2, :]
    x1, x2, slope_f, slope_g, inv_f, inv_g, norm_f, norm_g = pair_back(
        y1, y2, lambda: arrived(wbuf_f, sem_f), lambda: arrived(wbuf_g, sem_g), gain_f, gain_g
    )
    w_f, w_g = wbuf_f[...], wbuf_g[...]
    gz, gx2, delta_f, delta_g, back_f, back_g = grad_back(
        gy1, gy2, y1, x2, slope_f, slope_g, inv_f, inv_g, w_f, w_g, gain_f, gain_g
    )
    pair[:, 0:CH] = x1
    pair[:, CH : 2 * CH] = x2
    grad[:, 0:CH] = gz.astype(BF16)
    grad[:, CH : 2 * CH] = gx2.astype(BF16)
    gain_sums[0:1, :] = jnp.sum(back_f * x2 * inv_f, axis=0, keepdims=True)
    gain_sums[1:2, :] = jnp.sum(back_g * y1 * inv_g, axis=0, keepdims=True)
    contract = (((0,), (0,)), ((), ()))
    for at, n, d in ((0, norm_f, delta_f), (CH, norm_g, delta_g)):
        for k in range(0, CH, 256):
            part = lax.dot_general(n[:, k : k + 256], d, contract, preferred_element_type=F32)
            parts[k : k + 256, at : at + CH] = part.astype(BF16)


def run_owner(info, b, gains, own):
    vmem = pl.BlockSpec(memory_space=pltpu.VMEM)
    rows = b.shape[0]
    return pl.pallas_call(
        owner_kernel,
        out_shape=(
            jax.ShapeDtypeStruct((rows, 2 * CH), F32),
            jax.ShapeDtypeStruct((rows, 2 * CH), BF16),
            jax.ShapeDtypeStruct((CH, 2 * CH), BF16),
            jax.ShapeDtypeStruct((2, CH), F32),
        ),
        in_specs=[pl.BlockSpec(memory_space=pltpu.SMEM), vmem, vmem]
        + [pl.BlockSpec(memory_space=pltpu.HBM)] * N_REFS,
        out_specs=(vmem, vmem, vmem, vmem),
        scratch_shapes=[
            pltpu.VMEM((CH, CH), BF16),
            pltpu.VMEM((CH, CH), BF16),
            pltpu.SemaphoreType.DMA,
            pltpu.SemaphoreType.DMA,
        ],
        compiler_params=pltpu.CompilerParams(vmem_limit_bytes=52 * 2**20),
        cost_estimate=pl.CostEstimate(
            flops=12 * rows * CH * CH, bytes_accessed=12 * 2**20, transcendentals=0
        ),
        name="owner",
    )(info, b, gains, *own)


def shifted(array, axes, by, size):
    return lax.ppermute(array, axes, [(i, (i + by) % size) for i in range(size)])


def ring(block, axes, split):
    blocks = [block] + [None] * 7
    right = left = block
    for s in (1, 2, 3):
        right = shifted(right, axes, 1, 8)
        left = shifted(left, axes, -1, 8)
        blocks[s], blocks[8 - s] = right, left
    if not split:
        blocks[4] = shifted(right, axes, 1, 8)
        return blocks
    half = block.shape[0] // 2
    blocks[4] = shifted(right[:half], axes, 1, 8)
    return blocks + [shifted(left[half:], axes, -1, 8)]


Y = ("yh", "yl")


def swapped(array):
    return lax.ppermute(array, "c", [(0, 1), (1, 0)])


def gathered(f_shard, g_shard, gains):
    f_all = lax.all_gather(f_shard, ("yh", "yl", "z"), axis=0, tiled=True)
    g_blocks = ring(jnp.concatenate(ring(g_shard, "z", False)), Y, True)
    g_other = [swapped(b) for b in g_blocks]
    f_all, g_blocks, g_other, gains = lax.optimization_barrier((f_all, g_blocks, g_other, gains))
    return [f_all] + g_blocks, [swapped(f_all)] + g_other, gains


def shards(out_pair, out_grad, f_weight, g_weight, gains):
    x, yh, c, yl, z = (lax.axis_index(a).astype(jnp.int32) for a in ("x", "yh", "c", "yl", "z"))
    near = swapped(gains[0])
    chip_gains = jnp.where(c == 0, jnp.stack([gains[0], near]), jnp.stack([near, gains[0]]))
    far_gains = [shifted(chip_gains, "yh", by, 4) for by in (1, 2, 3)]
    all_gains = jnp.stack([chip_gains] + far_gains)
    own, other, all_gains = gathered(f_weight[0], g_weight[0], all_gains)
    at = (yh * 2 + c) * ROWS
    state = jnp.concatenate(
        [
            lax.dynamic_slice_in_dim(out_pair, at, ROWS, 0).astype(BF16),
            lax.dynamic_slice_in_dim(out_grad, at, ROWS, 0),
        ],
        axis=1,
    )
    bnd = jnp.zeros((LAYERS, ROWS, 4 * CH), BF16)
    y = yh * 2 + yl
    for stage in range(4):
        info = jnp.stack([(x == 3 - stage).astype(jnp.int32), c, y, z])
        bnd, out = run_stage(info, state, all_gains, own, other, bnd)
        if stage < 3:
            state = lax.ppermute(out, "x", [(3 - stage, 2 - stage)])
    mine = lax.all_to_all(bnd, ("yh", "c"), split_axis=0, concat_axis=0, tiled=True)
    mine = mine.reshape(LAYERS * ROWS, 4 * CH)
    pair, grad, parts, gain_part = run_owner(jnp.stack([y, z]), mine, gains[0], own)
    sums = lax.psum_scatter(parts, ("yl", "z"), scatter_dimension=0, tiled=True).astype(F32)
    gain_total = lax.psum(gain_part, ("yl", "z"))
    return (pair[None], grad[None], sums[None, :, :CH], sums[None, :, CH:], gain_total[None])


def solution(mesh):
    devices = mesh.devices.reshape(4, 4, 2, 2, 8)
    fine = Mesh(devices, ("x", "yh", "c", "yl", "z"))
    section, dp = ("x", "yh", "c"), ("yl", "z")
    return jax.shard_map(
        shards,
        mesh=fine,
        in_specs=(P(dp, None), P(dp, None), P(section, dp, None), P(section, dp, None), P(section, None, None)),
        out_specs=(
            P(section, dp, None),
            P(section, dp, None),
            P(section, dp, None),
            P(section, dp, None),
            P(section, None, None),
        ),
        check_vma=False,
    )
```

```python
import jax
import jax.numpy as jnp
from jax import lax
from jax.experimental import pallas as pl
from jax.experimental.pallas import tpu as pltpu
from jax.sharding import Mesh
from jax.sharding import PartitionSpec as P

offset = 0.25
CH = 1024
LAYERS = 8
ROWS = 16
F32, BF16 = jnp.float32, jnp.bfloat16


def silu_parts(pre):
    s = jax.nn.sigmoid(pre)
    return pre * s, s * (1.0 + pre * (1.0 - s))


def normalize(values, gain_row):
    inv = lax.rsqrt(jnp.mean(values * values, axis=-1, keepdims=True) + offset)
    return (values * inv * gain_row).astype(BF16), inv


def norm_back(values, inv, gain_row, upstream):
    weighted = gain_row * upstream
    return inv * weighted - values * (inv * inv * inv) * jnp.mean(
        weighted * values, axis=-1, keepdims=True
    )


def times(a, w):
    return jnp.dot(a, w, preferred_element_type=F32)


def times_transposed(a, w):
    return lax.dot_general(a, w, (((1,), (1,)), ((), ())), preferred_element_type=F32)


def pair_back(y1, y2, w_f, w_g, gain_f, gain_g):
    norm_g, inv_g = normalize(y1, gain_g)
    act_g, slope_g = silu_parts(times(norm_g, w_g()))
    x2 = y2 - act_g
    norm_f, inv_f = normalize(x2, gain_f)
    act_f, slope_f = silu_parts(times(norm_f, w_f()))
    return y1 - act_f, x2, slope_f, slope_g, inv_f, inv_g, norm_f, norm_g


def grad_back(gy1, gy2, y1, x2, slope_f, slope_g, inv_f, inv_g, w_f, w_g, gain_f, gain_g):
    delta_g = (gy2 * slope_g).astype(BF16)
    back_g = times_transposed(delta_g, w_g())
    gz = gy1 + norm_back(y1, inv_g, gain_g, back_g)
    delta_f = (gz * slope_f).astype(BF16)
    back_f = times_transposed(delta_f, w_f())
    gx2 = gy2 + norm_back(x2, inv_f, gain_f, back_f)
    return gz, gx2, delta_f, delta_g, back_f, back_g


def fetch(j, info, own, other, w_f, w_g, sem_f, sem_g):
    layer = LAYERS - 1 - j
    slot = lax.rem(j, 3)
    rows = pl.ds((layer // 2) * CH, CH)
    mine = lax.rem(layer, 2) == info[1]
    for want, src in ((mine, own), (jnp.logical_not(mine), other)):

        @pl.when(want)
        def _(src=src):
            pltpu.make_async_copy(src.at[rows, pl.ds(CH, CH)], w_g.at[slot], sem_g.at[slot]).start()
            pltpu.make_async_copy(src.at[rows, pl.ds(0, CH)], w_f.at[slot], sem_f.at[slot]).start()


def arrived(j, src, buf, sem):
    slot = lax.rem(j, 3)
    pltpu.make_async_copy(src.at[pl.ds(0, CH), pl.ds(0, CH)], buf.at[slot], sem.at[slot]).wait()
    return buf[slot]


def gain_rows(j, info, gains):
    layer = LAYERS - 1 - j
    far = lax.rem(info[2] - layer // 2 + 4, 4)
    part = lax.rem(layer, 2)
    return gains[far, part, 0:1, :], gains[far, part, 1:2, :]


def pair_kernel(info, state, gains, own, other, bnd_in, bnd, kept, out, w_f, w_g, bbuf, kbuf, sem_f, sem_g, bsem, ksem):
    del bnd_in

    def leave(j):
        layer = LAYERS - 1 - j
        pltpu.make_async_copy(bbuf.at[layer], bnd.at[layer], bsem).start()
        pltpu.make_async_copy(kbuf.at[j], kept.at[j], ksem).start()

    @pl.when(info[0] == 1)
    def _():
        fetch(0, info, own, other, w_f, w_g, sem_f, sem_g)
        fetch(1, info, own, other, w_f, w_g, sem_f, sem_g)

        def step(j, carry):
            y1, y2 = carry
            layer = LAYERS - 1 - j

            @pl.when(j < LAYERS - 2)
            def _():
                fetch(j + 2, info, own, other, w_f, w_g, sem_f, sem_g)

            bbuf[layer, :, 0:CH] = y1.astype(BF16)
            bbuf[layer, :, CH : 2 * CH] = y2.astype(BF16)
            gain_f, gain_g = gain_rows(j, info, gains)
            x1, x2, slope_f, slope_g = pair_back(
                y1,
                y2,
                lambda: arrived(j, own, w_f, sem_f),
                lambda: arrived(j, own, w_g, sem_g),
                gain_f,
                gain_g,
            )[:4]
            for k, v in enumerate((y1, x2, slope_f, slope_g)):
                kbuf[j, :, k * CH : (k + 1) * CH] = v

            @pl.when(j > 0)
            def _():
                leave(j - 1)

            return x1, x2

        first = tuple(state[:, k * CH : (k + 1) * CH].astype(F32) for k in range(2))
        last = lax.fori_loop(0, LAYERS, step, first)
        for k in range(2):
            out[:, k * CH : (k + 1) * CH] = last[k].astype(BF16)
        leave(LAYERS - 1)
        pltpu.make_async_copy(bbuf, bnd, bsem).wait()
        pltpu.make_async_copy(kbuf, kept, ksem).wait()


def grad_kernel(info, state, gains, own, other, kept, bnd_in, bnd, out, w_f, w_g, bbuf, kbuf, sem_f, sem_g, bsem, ksem):
    del bnd_in

    @pl.when(info[0] == 1)
    def _():
        pltpu.make_async_copy(kept.at[0], kbuf.at[0], ksem.at[0]).start()
        fetch(0, info, own, other, w_f, w_g, sem_f, sem_g)
        pltpu.make_async_copy(kept.at[1], kbuf.at[1], ksem.at[1]).start()
        fetch(1, info, own, other, w_f, w_g, sem_f, sem_g)

        def step(j, carry):
            gy1, gy2 = carry
            layer = LAYERS - 1 - j
            at = lax.rem(j, 3)

            @pl.when(j < LAYERS - 2)
            def _():
                ahead = lax.rem(j + 2, 3)
                pltpu.make_async_copy(kept.at[j + 2], kbuf.at[ahead], ksem.at[ahead]).start()
                fetch(j + 2, info, own, other, w_f, w_g, sem_f, sem_g)

            bbuf[layer, :, 0:CH] = gy1.astype(BF16)
            bbuf[layer, :, CH : 2 * CH] = gy2.astype(BF16)
            pltpu.make_async_copy(kept.at[0], kbuf.at[at], ksem.at[at]).wait()
            y1, x2, slope_f, slope_g = (kbuf[at, :, k * CH : (k + 1) * CH] for k in range(4))
            inv_f = lax.rsqrt(jnp.mean(x2 * x2, axis=-1, keepdims=True) + offset)
            inv_g = lax.rsqrt(jnp.mean(y1 * y1, axis=-1, keepdims=True) + offset)
            gz, gx2 = grad_back(
                gy1,
                gy2,
                y1,
                x2,
                slope_f,
                slope_g,
                inv_f,
                inv_g,
                lambda: arrived(j, own, w_f, sem_f),
                lambda: arrived(j, own, w_g, sem_g),
                *gain_rows(j, info, gains),
            )[:2]
            pltpu.make_async_copy(bbuf.at[layer], bnd.at[layer], bsem).start()
            return gz.astype(BF16).astype(F32), gx2.astype(BF16).astype(F32)

        first = tuple(state[:, k * CH : (k + 1) * CH].astype(F32) for k in range(2))
        last = lax.fori_loop(0, LAYERS, step, first)
        for k in range(2):
            out[:, k * CH : (k + 1) * CH] = last[k].astype(BF16)
        pltpu.make_async_copy(bbuf, bnd, bsem).wait()


BND = jax.ShapeDtypeStruct((LAYERS, ROWS, 2 * CH), BF16)
KEPT = jax.ShapeDtypeStruct((LAYERS, ROWS, 4 * CH), F32)
STATE = jax.ShapeDtypeStruct((ROWS, 2 * CH), BF16)
VMEM = pl.BlockSpec(memory_space=pltpu.VMEM)
HBM = pl.BlockSpec(memory_space=pltpu.HBM)
SMEM = pl.BlockSpec(memory_space=pltpu.SMEM)
WEIGHT_BUFFERS = [
    pltpu.VMEM((3, CH, CH), BF16),
    pltpu.VMEM((3, CH, CH), BF16),
    pltpu.VMEM(BND.shape, BF16),
]
WEIGHT_SEMS = [pltpu.SemaphoreType.DMA((3,)), pltpu.SemaphoreType.DMA((3,)), pltpu.SemaphoreType.DMA]
STAGE_PARAMS = pltpu.CompilerParams(
    vmem_limit_bytes=48 * 2**20
)
STAGE_COST = pl.CostEstimate(
    flops=4 * 8 * ROWS * CH * CH, bytes_accessed=32 * 2**20, transcendentals=0
)


def run_pairs(info, state, gains, own, other, bnd):
    return pl.pallas_call(
        pair_kernel,
        out_shape=(BND, KEPT, STATE),
        in_specs=[SMEM, VMEM, VMEM, HBM, HBM, HBM],
        out_specs=(HBM, HBM, VMEM),
        scratch_shapes=WEIGHT_BUFFERS
        + [pltpu.VMEM(KEPT.shape, F32)]
        + WEIGHT_SEMS
        + [pltpu.SemaphoreType.DMA],
        input_output_aliases={5: 0},
        compiler_params=STAGE_PARAMS,
        cost_estimate=STAGE_COST,
        name="pairs",
    )(info, state, gains, own, other, bnd)


def run_grads(info, state, gains, own, other, kept, bnd):
    return pl.pallas_call(
        grad_kernel,
        out_shape=(BND, STATE),
        in_specs=[SMEM, VMEM, VMEM, HBM, HBM, HBM, HBM],
        out_specs=(HBM, VMEM),
        scratch_shapes=WEIGHT_BUFFERS
        + [pltpu.VMEM((3, ROWS, 4 * CH), F32)]
        + WEIGHT_SEMS
        + [pltpu.SemaphoreType.DMA((3,))],
        input_output_aliases={6: 0},
        compiler_params=STAGE_PARAMS,
        cost_estimate=STAGE_COST,
        name="grads",
    )(info, state, gains, own, other, kept, bnd)


def owner_kernel(info, pb, gb, gains, own, pair, grad, parts, gain_sums, wbuf_f, wbuf_g, sem_f, sem_g):
    rows = pl.ds(info[0] * CH, CH)
    copy_g = pltpu.make_async_copy(own.at[rows, pl.ds(CH, CH)], wbuf_g, sem_g)
    copy_f = pltpu.make_async_copy(own.at[rows, pl.ds(0, CH)], wbuf_f, sem_f)
    copy_g.start()
    copy_f.start()

    def landed(copy, buf):
        copy.wait()
        return buf[...]

    y1, y2 = (pb[:, k * CH : (k + 1) * CH].astype(F32) for k in range(2))
    gy1, gy2 = (gb[:, k * CH : (k + 1) * CH].astype(F32) for k in range(2))
    gain_f, gain_g = gains[0:1, :], gains[1:2, :]
    x1, x2, slope_f, slope_g, inv_f, inv_g, norm_f, norm_g = pair_back(
        y1, y2, lambda: landed(copy_f, wbuf_f), lambda: landed(copy_g, wbuf_g), gain_f, gain_g
    )
    gz, gx2, delta_f, delta_g, back_f, back_g = grad_back(
        gy1,
        gy2,
        y1,
        x2,
        slope_f,
        slope_g,
        inv_f,
        inv_g,
        lambda: wbuf_f[...],
        lambda: wbuf_g[...],
        gain_f,
        gain_g,
    )
    pair[:, 0:CH] = x1
    pair[:, CH : 2 * CH] = x2
    grad[:, 0:CH] = gz.astype(BF16)
    grad[:, CH : 2 * CH] = gx2.astype(BF16)
    gain_sums[0:1, :] = jnp.sum(back_f * x2 * inv_f, axis=0, keepdims=True)
    gain_sums[1:2, :] = jnp.sum(back_g * y1 * inv_g, axis=0, keepdims=True)
    contract = (((0,), (0,)), ((), ()))
    for at, n, d in ((0, norm_f, delta_f), (CH, norm_g, delta_g)):
        for k in range(0, CH, 256):
            part = lax.dot_general(n[:, k : k + 256], d, contract, preferred_element_type=F32)
            parts[k : k + 256, at : at + CH] = part.astype(BF16)


def run_owner(info, pb, gb, gains, own):
    vmem = VMEM
    rows = pb.shape[0]
    return pl.pallas_call(
        owner_kernel,
        out_shape=(
            jax.ShapeDtypeStruct((rows, 2 * CH), F32),
            jax.ShapeDtypeStruct((rows, 2 * CH), BF16),
            jax.ShapeDtypeStruct((CH, 2 * CH), BF16),
            jax.ShapeDtypeStruct((2, CH), F32),
        ),
        in_specs=[SMEM, vmem, vmem, vmem, HBM],
        out_specs=(vmem, vmem, vmem, vmem),
        scratch_shapes=[
            pltpu.VMEM((CH, CH), BF16),
            pltpu.VMEM((CH, CH), BF16),
            pltpu.SemaphoreType.DMA,
            pltpu.SemaphoreType.DMA,
        ],
        compiler_params=pltpu.CompilerParams(vmem_limit_bytes=52 * 2**20),
        cost_estimate=pl.CostEstimate(
            flops=12 * rows * CH * CH, bytes_accessed=12 * 2**20, transcendentals=0
        ),
        name="owner",
    )(info, pb, gb, gains, own)


def swapped(array):
    return lax.ppermute(array, "c", [(0, 1), (1, 0)])


def to_owner(bnd):
    mine = lax.all_to_all(bnd, ("yh", "c"), split_axis=0, concat_axis=0, tiled=True)
    return mine.reshape(LAYERS * ROWS, 2 * CH)


def shards(out_pair, out_grad, f_weight, g_weight, gains):
    x, yh, c = (lax.axis_index(a).astype(jnp.int32) for a in ("x", "yh", "c"))
    shard = jnp.concatenate([f_weight[0], g_weight[0]], axis=1)
    own = lax.all_gather(shard, ("yh", "yl", "z"), axis=0, tiled=True)
    near = swapped(gains[0])
    chip_gains = jnp.where(c == 0, jnp.stack([gains[0], near]), jnp.stack([near, gains[0]]))
    far_gains = [
        lax.ppermute(chip_gains, "yh", [(i, (i + by) % 4) for i in range(4)]) for by in (1, 2, 3)
    ]
    all_gains = jnp.stack([chip_gains] + far_gains)
    at = (yh * 2 + c) * ROWS
    pairs = lax.dynamic_slice_in_dim(out_pair, at, ROWS, 0).astype(BF16)
    grads = lax.dynamic_slice_in_dim(out_grad, at, ROWS, 0)
    own, all_gains, pairs, grads = lax.optimization_barrier((own, all_gains, pairs, grads))
    other = swapped(own)
    infos = [jnp.stack([(x == 3 - stage).astype(jnp.int32), c, yh]) for stage in range(4)]
    pb = gb = jnp.zeros(BND.shape, BF16)
    for stage in range(4):
        hop = [(3 - stage, 2 - stage)]
        pb, kept, next_pairs = run_pairs(infos[stage], pairs, all_gains, own, other, pb)
        if stage < 3:
            pairs = lax.ppermute(next_pairs, "x", hop)
        gb, next_grads = run_grads(infos[stage], grads, all_gains, own, other, kept, gb)
        if stage < 3:
            grads = lax.ppermute(next_grads, "x", hop)
            pairs, gb = lax.optimization_barrier((pairs, gb))
    pair, grad, parts, gain_part = run_owner(
        jnp.reshape(yh, (1,)), to_owner(pb), to_owner(gb), gains[0], own
    )
    sums = lax.psum_scatter(parts, ("yl", "z"), scatter_dimension=0, tiled=True).astype(F32)
    gain_total = lax.psum(gain_part, ("yl", "z"))
    return (pair[None], grad[None], sums[None, :, :CH], sums[None, :, CH:], gain_total[None])


def solution(mesh):
    devices = mesh.devices.reshape(4, 4, 2, 2, 8)
    fine = Mesh(devices, ("x", "yh", "c", "yl", "z"))
    section, dp = ("x", "yh", "c"), ("yl", "z")
    return jax.shard_map(
        shards,
        mesh=fine,
        in_specs=(P(dp, None), P(dp, None), P(section, dp, None), P(section, dp, None), P(section, None, None)),
        out_specs=(
            P(section, dp, None),
            P(section, dp, None),
            P(section, dp, None),
            P(section, dp, None),
            P(section, None, None),
        ),
        check_vma=False,
    )
```

```python
import jax
import jax.numpy as jnp
from jax import lax
from jax.experimental import pallas as pl
from jax.experimental.pallas import tpu as pltpu
from jax.sharding import Mesh
from jax.sharding import PartitionSpec as P

offset = 0.25
CH = 1024
LAYERS = 8
ROWS = 16
F32, BF16 = jnp.float32, jnp.bfloat16
PAIRS, GRADS = pl.ds(0, 2 * CH), pl.ds(2 * CH, 2 * CH)


def silu_parts(pre):
    s = jax.nn.sigmoid(pre)
    return pre * s, s * (1.0 + pre * (1.0 - s))


def normalize(values, gain_row):
    inv = lax.rsqrt(jnp.mean(values * values, axis=-1, keepdims=True) + offset)
    return (values * inv * gain_row).astype(BF16), inv


def norm_back(values, inv, gain_row, upstream):
    weighted = gain_row * upstream
    return inv * weighted - values * (inv * inv * inv) * jnp.mean(
        weighted * values, axis=-1, keepdims=True
    )


def times(a, w):
    return jnp.dot(a, w, preferred_element_type=F32)


def times_transposed(a, w):
    return lax.dot_general(a, w, (((1,), (1,)), ((), ())), preferred_element_type=F32)


def pair_back(y1, y2, w_f, w_g, gain_f, gain_g):
    norm_g, inv_g = normalize(y1, gain_g)
    act_g, slope_g = silu_parts(times(norm_g, w_g()))
    x2 = y2 - act_g
    norm_f, inv_f = normalize(x2, gain_f)
    act_f, slope_f = silu_parts(times(norm_f, w_f()))
    return y1 - act_f, x2, slope_f, slope_g, inv_f, inv_g, norm_f, norm_g


def grad_back(gy1, gy2, y1, x2, slope_f, slope_g, inv_f, inv_g, w_f, w_g, gain_f, gain_g):
    delta_g = (gy2 * slope_g).astype(BF16)
    back_g = times_transposed(delta_g, w_g())
    gz = gy1 + norm_back(y1, inv_g, gain_g, back_g)
    delta_f = (gz * slope_f).astype(BF16)
    back_f = times_transposed(delta_f, w_f())
    gx2 = gy2 + norm_back(x2, inv_f, gain_f, back_f)
    return gz, gx2, delta_f, delta_g, back_f, back_g


def row_scale(values):
    return lax.rsqrt(jnp.mean(values * values, axis=-1, keepdims=True) + offset)


def scaled_after(values, gain_row, w):
    return row_scale(values) * times((values * gain_row).astype(BF16), w)


def grad_through(upper, delta, values, pre, w, gain_row):
    inv = row_scale(values)
    mean = jnp.mean(delta.astype(F32) * pre, axis=-1, keepdims=True)
    rest = upper - values * (inv * inv * mean)
    return rest + (inv * gain_row) * times_transposed(delta, w)


def fetch(j, info, own, other, w_f, w_g, sem_f, sem_g):
    layer = LAYERS - 1 - j
    slot = lax.rem(j, 3)
    rows = pl.ds((layer // 2) * CH, CH)
    mine = lax.rem(layer, 2) == info[1]
    for want, src in ((mine, own), (jnp.logical_not(mine), other)):

        @pl.when(want)
        def _(src=src):
            pltpu.make_async_copy(src.at[rows, pl.ds(CH, CH)], w_g.at[slot], sem_g.at[slot]).start()
            pltpu.make_async_copy(src.at[rows, pl.ds(0, CH)], w_f.at[slot], sem_f.at[slot]).start()


def arrived(j, src, buf, sem):
    slot = lax.rem(j, 3)
    pltpu.make_async_copy(src.at[pl.ds(0, CH), pl.ds(0, CH)], buf.at[slot], sem.at[slot]).wait()
    return buf[slot]


def gain_rows(j, info, gains):
    layer = LAYERS - 1 - j
    far = lax.rem(info[2] - layer // 2 + 4, 4)
    part = lax.rem(layer, 2)
    return gains[far, part, 0:1, :], gains[far, part, 1:2, :]


def pair_kernel(info, state, gains, own, other, bnd_in, bnd, kept, out, w_f, w_g, bbuf, kbuf, sem_f, sem_g, bsem, ksem):
    del bnd_in

    def leave(j):
        layer = LAYERS - 1 - j
        pltpu.make_async_copy(bbuf.at[layer], bnd.at[layer, :, PAIRS], bsem).start()
        pltpu.make_async_copy(kbuf.at[j], kept.at[j], ksem).start()

    @pl.when(info[0] == 1)
    def _():
        fetch(0, info, own, other, w_f, w_g, sem_f, sem_g)
        fetch(1, info, own, other, w_f, w_g, sem_f, sem_g)

        def step(j, carry):
            y1, y2 = carry
            layer = LAYERS - 1 - j

            @pl.when(j < LAYERS - 2)
            def _():
                fetch(j + 2, info, own, other, w_f, w_g, sem_f, sem_g)

            bbuf[layer, :, 0:CH] = y1.astype(BF16)
            bbuf[layer, :, CH : 2 * CH] = y2.astype(BF16)
            gain_f, gain_g = gain_rows(j, info, gains)
            pre_g = scaled_after(y1, gain_g, arrived(j, own, w_g, sem_g))
            act_g, slope_g = silu_parts(pre_g)
            x2 = y2 - act_g
            pre_f = scaled_after(x2, gain_f, arrived(j, own, w_f, sem_f))
            act_f, slope_f = silu_parts(pre_f)
            x1 = y1 - act_f
            for k, v in enumerate((y1, x2, slope_f, slope_g, pre_f, pre_g)):
                kbuf[j, :, k * CH : (k + 1) * CH] = v

            @pl.when(j > 0)
            def _():
                leave(j - 1)

            return x1, x2

        first = tuple(state[:, k * CH : (k + 1) * CH].astype(F32) for k in range(2))
        last = lax.fori_loop(0, LAYERS, step, first)
        for k in range(2):
            out[:, k * CH : (k + 1) * CH] = last[k].astype(BF16)
        leave(LAYERS - 1)
        pltpu.make_async_copy(bbuf, bnd.at[:, :, PAIRS], bsem).wait()
        pltpu.make_async_copy(kbuf, kept, ksem).wait()


def grad_kernel(info, state, gains, own, other, kept, bnd_in, bnd, out, w_f, w_g, bbuf, kbuf, sem_f, sem_g, bsem, ksem):
    del bnd_in

    @pl.when(info[0] == 1)
    def _():
        pltpu.make_async_copy(kept.at[0], kbuf.at[0], ksem.at[0]).start()
        fetch(0, info, own, other, w_f, w_g, sem_f, sem_g)
        pltpu.make_async_copy(kept.at[1], kbuf.at[1], ksem.at[1]).start()
        fetch(1, info, own, other, w_f, w_g, sem_f, sem_g)

        def step(j, carry):
            gy1, gy2 = carry
            layer = LAYERS - 1 - j
            at = lax.rem(j, 3)

            @pl.when(j < LAYERS - 2)
            def _():
                ahead = lax.rem(j + 2, 3)
                pltpu.make_async_copy(kept.at[j + 2], kbuf.at[ahead], ksem.at[ahead]).start()
                fetch(j + 2, info, own, other, w_f, w_g, sem_f, sem_g)

            bbuf[layer, :, 0:CH] = gy1.astype(BF16)
            bbuf[layer, :, CH : 2 * CH] = gy2.astype(BF16)
            pltpu.make_async_copy(kept.at[0], kbuf.at[at], ksem.at[at]).wait()
            y1, x2, slope_f, slope_g, pre_f, pre_g = (
                kbuf[at, :, k * CH : (k + 1) * CH] for k in range(6)
            )
            gain_f, gain_g = gain_rows(j, info, gains)
            delta_g = (gy2 * slope_g).astype(BF16)
            gz = grad_through(gy1, delta_g, y1, pre_g, arrived(j, own, w_g, sem_g), gain_g)
            delta_f = (gz * slope_f).astype(BF16)
            gx2 = grad_through(gy2, delta_f, x2, pre_f, arrived(j, own, w_f, sem_f), gain_f)
            pltpu.make_async_copy(bbuf.at[layer], bnd.at[layer, :, GRADS], bsem).start()
            return gz.astype(BF16).astype(F32), gx2.astype(BF16).astype(F32)

        first = tuple(state[:, k * CH : (k + 1) * CH].astype(F32) for k in range(2))
        last = lax.fori_loop(0, LAYERS, step, first)
        for k in range(2):
            out[:, k * CH : (k + 1) * CH] = last[k].astype(BF16)
        pltpu.make_async_copy(bbuf, bnd.at[:, :, GRADS], bsem).wait()


BND = jax.ShapeDtypeStruct((LAYERS, ROWS, 4 * CH), BF16)
KEPT = jax.ShapeDtypeStruct((LAYERS, ROWS, 6 * CH), F32)
STATE = jax.ShapeDtypeStruct((ROWS, 2 * CH), BF16)
VMEM = pl.BlockSpec(memory_space=pltpu.VMEM)
HBM = pl.BlockSpec(memory_space=pltpu.HBM)
SMEM = pl.BlockSpec(memory_space=pltpu.SMEM)
WEIGHT_BUFFERS = [
    pltpu.VMEM((3, CH, CH), BF16),
    pltpu.VMEM((3, CH, CH), BF16),
    pltpu.VMEM((LAYERS, ROWS, 2 * CH), BF16),
]
WEIGHT_SEMS = [pltpu.SemaphoreType.DMA((3,)), pltpu.SemaphoreType.DMA((3,)), pltpu.SemaphoreType.DMA]
STAGE_PARAMS = pltpu.CompilerParams(
    vmem_limit_bytes=48 * 2**20
)
STAGE_COST = pl.CostEstimate(
    flops=4 * 8 * ROWS * CH * CH, bytes_accessed=32 * 2**20, transcendentals=0
)


def run_pairs(info, state, gains, own, other, bnd):
    return pl.pallas_call(
        pair_kernel,
        out_shape=(BND, KEPT, STATE),
        in_specs=[SMEM, VMEM, VMEM, HBM, HBM, HBM],
        out_specs=(HBM, HBM, VMEM),
        scratch_shapes=WEIGHT_BUFFERS
        + [pltpu.VMEM(KEPT.shape, F32)]
        + WEIGHT_SEMS
        + [pltpu.SemaphoreType.DMA],
        input_output_aliases={5: 0},
        compiler_params=STAGE_PARAMS,
        cost_estimate=STAGE_COST,
        name="pairs",
    )(info, state, gains, own, other, bnd)


def run_grads(info, state, gains, own, other, kept, bnd):
    return pl.pallas_call(
        grad_kernel,
        out_shape=(BND, STATE),
        in_specs=[SMEM, VMEM, VMEM, HBM, HBM, HBM, HBM],
        out_specs=(HBM, VMEM),
        scratch_shapes=WEIGHT_BUFFERS
        + [pltpu.VMEM((3, ROWS, 6 * CH), F32)]
        + WEIGHT_SEMS
        + [pltpu.SemaphoreType.DMA((3,))],
        input_output_aliases={6: 0},
        compiler_params=STAGE_PARAMS,
        cost_estimate=STAGE_COST,
        name="grads",
    )(info, state, gains, own, other, kept, bnd)


def owner_kernel(info, b, gains, own, pair, grad, parts, gain_sums, wbuf_f, wbuf_g, sem_f, sem_g):
    rows = pl.ds(info[0] * CH, CH)
    copy_g = pltpu.make_async_copy(own.at[rows, pl.ds(CH, CH)], wbuf_g, sem_g)
    copy_f = pltpu.make_async_copy(own.at[rows, pl.ds(0, CH)], wbuf_f, sem_f)
    copy_g.start()
    copy_f.start()

    def landed(copy, buf):
        copy.wait()
        return buf[...]

    y1, y2, gy1, gy2 = (b[:, k * CH : (k + 1) * CH].astype(F32) for k in range(4))
    gain_f, gain_g = gains[0:1, :], gains[1:2, :]
    x1, x2, slope_f, slope_g, inv_f, inv_g, norm_f, norm_g = pair_back(
        y1, y2, lambda: landed(copy_f, wbuf_f), lambda: landed(copy_g, wbuf_g), gain_f, gain_g
    )
    gz, gx2, delta_f, delta_g, back_f, back_g = grad_back(
        gy1,
        gy2,
        y1,
        x2,
        slope_f,
        slope_g,
        inv_f,
        inv_g,
        lambda: wbuf_f[...],
        lambda: wbuf_g[...],
        gain_f,
        gain_g,
    )
    pair[:, 0:CH] = x1
    pair[:, CH : 2 * CH] = x2
    grad[:, 0:CH] = gz.astype(BF16)
    grad[:, CH : 2 * CH] = gx2.astype(BF16)
    gain_sums[0:1, :] = jnp.sum(back_f * x2 * inv_f, axis=0, keepdims=True)
    gain_sums[1:2, :] = jnp.sum(back_g * y1 * inv_g, axis=0, keepdims=True)
    contract = (((0,), (0,)), ((), ()))
    for at, n, d in ((0, norm_f, delta_f), (CH, norm_g, delta_g)):
        for k in range(0, CH, 256):
            part = lax.dot_general(n[:, k : k + 256], d, contract, preferred_element_type=F32)
            for q in range(4):
                yl, z = (k // 64 + q) // 8, (k // 64 + q) % 8
                rows = pl.ds((z * 2 + yl) * 64, 64)
                parts[rows, at : at + CH] = part[q * 64 : (q + 1) * 64].astype(BF16)


def run_owner(info, b, gains, own):
    vmem = VMEM
    rows = b.shape[0]
    return pl.pallas_call(
        owner_kernel,
        out_shape=(
            jax.ShapeDtypeStruct((rows, 2 * CH), F32),
            jax.ShapeDtypeStruct((rows, 2 * CH), BF16),
            jax.ShapeDtypeStruct((CH, 2 * CH), BF16),
            jax.ShapeDtypeStruct((2, CH), F32),
        ),
        in_specs=[SMEM, vmem, vmem, HBM],
        out_specs=(vmem, vmem, vmem, vmem),
        scratch_shapes=[
            pltpu.VMEM((CH, CH), BF16),
            pltpu.VMEM((CH, CH), BF16),
            pltpu.SemaphoreType.DMA,
            pltpu.SemaphoreType.DMA,
        ],
        compiler_params=pltpu.CompilerParams(vmem_limit_bytes=52 * 2**20),
        cost_estimate=pl.CostEstimate(
            flops=12 * rows * CH * CH, bytes_accessed=12 * 2**20, transcendentals=0
        ),
        name="owner",
    )(info, b, gains, own)


def swapped(array):
    return lax.ppermute(array, "c", [(0, 1), (1, 0)])


def shards(out_pair, out_grad, f_weight, g_weight, gains):
    x, yh, c = (lax.axis_index(a).astype(jnp.int32) for a in ("x", "yh", "c"))
    shard = jnp.concatenate([f_weight[0], g_weight[0]], axis=1)
    own = lax.all_gather(shard, ("yh", "yl", "z"), axis=0, tiled=True)
    near = swapped(gains[0])
    chip_gains = jnp.where(c == 0, jnp.stack([gains[0], near]), jnp.stack([near, gains[0]]))
    far_gains = [
        lax.ppermute(chip_gains, "yh", [(i, (i + by) % 4) for i in range(4)]) for by in (1, 2, 3)
    ]
    all_gains = jnp.stack([chip_gains] + far_gains)
    at = (yh * 2 + c) * ROWS
    pairs = lax.dynamic_slice_in_dim(out_pair, at, ROWS, 0).astype(BF16)
    grads = lax.dynamic_slice_in_dim(out_grad, at, ROWS, 0)
    own, all_gains, pairs, grads = lax.optimization_barrier((own, all_gains, pairs, grads))
    other = swapped(own)
    infos = [jnp.stack([(x == 3 - stage).astype(jnp.int32), c, yh]) for stage in range(4)]
    bnd = jnp.zeros(BND.shape, BF16)
    for stage in range(4):
        hop = [(3 - stage, 2 - stage)]
        bnd, kept, next_pairs = run_pairs(infos[stage], pairs, all_gains, own, other, bnd)
        if stage < 3:
            pairs = lax.ppermute(next_pairs, "x", hop)
        bnd, next_grads = run_grads(infos[stage], grads, all_gains, own, other, kept, bnd)
        if stage < 3:
            grads = lax.ppermute(next_grads, "x", hop)
    mine = lax.all_to_all(bnd, ("yh", "c"), split_axis=0, concat_axis=0, tiled=True)
    mine = mine.reshape(LAYERS * ROWS, 4 * CH)
    pair, grad, parts, gain_part = run_owner(jnp.reshape(yh, (1,)), mine, gains[0], own)
    sums = lax.psum_scatter(parts, "z", scatter_dimension=0, tiled=True)
    gain_total = lax.psum(gain_part, ("yl", "z"))
    sums, gain_total = lax.optimization_barrier((sums, gain_total))
    sums = sums.reshape(2, 64, 2 * CH)
    first = lax.axis_index("yl") == 0
    theirs = lax.ppermute(jnp.where(first, sums[1], sums[0]), "yl", [(0, 1), (1, 0)])
    sums = jnp.where(first, sums[0], sums[1]).astype(F32) + theirs.astype(F32)
    return (pair[None], grad[None], sums[None, :, :CH], sums[None, :, CH:], gain_total[None])


def solution(mesh):
    devices = mesh.devices.reshape(4, 4, 2, 2, 8)
    fine = Mesh(devices, ("x", "yh", "c", "yl", "z"))
    section, dp = ("x", "yh", "c"), ("yl", "z")
    return jax.shard_map(
        shards,
        mesh=fine,
        in_specs=(P(dp, None), P(dp, None), P(section, dp, None), P(section, dp, None), P(section, None, None)),
        out_specs=(
            P(section, dp, None),
            P(section, dp, None),
            P(section, dp, None),
            P(section, dp, None),
            P(section, None, None),
        ),
        check_vma=False,
    )
```

```python
import jax
import jax.numpy as jnp
from jax import lax
from jax.experimental import pallas as pl
from jax.experimental.pallas import tpu as pltpu
from jax.sharding import Mesh
from jax.sharding import PartitionSpec as P

offset = 0.25
CH = 1024
LAYERS = 8
ROWS = 16
F32, BF16 = jnp.float32, jnp.bfloat16


def silu_parts(pre):
    s = jax.nn.sigmoid(pre)
    return pre * s, s * (1.0 + pre * (1.0 - s))


def normalize(values, gain_row):
    inv = lax.rsqrt(jnp.mean(values * values, axis=-1, keepdims=True) + offset)
    return (values * inv * gain_row).astype(BF16), inv


def norm_back(values, inv, gain_row, upstream):
    weighted = gain_row * upstream
    return inv * weighted - values * (inv * inv * inv) * jnp.mean(
        weighted * values, axis=-1, keepdims=True
    )


def times(a, w):
    return jnp.dot(a, w, preferred_element_type=F32)


def times_transposed(a, w):
    return lax.dot_general(a, w, (((1,), (1,)), ((), ())), preferred_element_type=F32)


def pair_back(y1, y2, w_f, w_g, gain_f, gain_g):
    norm_g, inv_g = normalize(y1, gain_g)
    act_g, slope_g = silu_parts(times(norm_g, w_g()))
    x2 = y2 - act_g
    norm_f, inv_f = normalize(x2, gain_f)
    act_f, slope_f = silu_parts(times(norm_f, w_f()))
    return y1 - act_f, x2, slope_f, slope_g, inv_f, inv_g, norm_f, norm_g


def grad_back(gy1, gy2, y1, x2, slope_f, slope_g, inv_f, inv_g, w_f, w_g, gain_f, gain_g):
    delta_g = (gy2 * slope_g).astype(BF16)
    back_g = times_transposed(delta_g, w_g())
    gz = gy1 + norm_back(y1, inv_g, gain_g, back_g)
    delta_f = (gz * slope_f).astype(BF16)
    back_f = times_transposed(delta_f, w_f())
    gx2 = gy2 + norm_back(x2, inv_f, gain_f, back_f)
    return gz, gx2, delta_f, delta_g, back_f, back_g


def row_scale(values):
    return lax.rsqrt(jnp.mean(values * values, axis=-1, keepdims=True) + offset)


def scaled_after(values, gain_row, w):
    return row_scale(values) * times((values * gain_row).astype(BF16), w)


def grad_through(upper, delta, values, pre, w, gain_row):
    inv = row_scale(values)
    mean = jnp.mean(delta.astype(F32) * pre, axis=-1, keepdims=True)
    rest = upper - values * (inv * inv * mean)
    return rest + (inv * gain_row) * times_transposed(delta, w)


def fetch(j, info, own, other, w_f, w_g, sem_f, sem_g):
    layer = LAYERS - 1 - j
    slot = lax.rem(j, 3)
    rows = pl.ds((layer // 2) * CH, CH)
    mine = lax.rem(layer, 2) == info[1]
    for want, src in ((mine, own), (jnp.logical_not(mine), other)):

        @pl.when(want)
        def _(src=src):
            pltpu.make_async_copy(src.at[rows, pl.ds(CH, CH)], w_g.at[slot], sem_g.at[slot]).start()
            pltpu.make_async_copy(src.at[rows, pl.ds(0, CH)], w_f.at[slot], sem_f.at[slot]).start()


def arrived(j, src, buf, sem):
    slot = lax.rem(j, 3)
    pltpu.make_async_copy(src.at[pl.ds(0, CH), pl.ds(0, CH)], buf.at[slot], sem.at[slot]).wait()
    return buf[slot]


def gain_rows(j, info, gains):
    layer = LAYERS - 1 - j
    far = lax.rem(info[2] - layer // 2 + 4, 4)
    part = lax.rem(layer, 2)
    return gains[far, part, 0:1, :], gains[far, part, 1:2, :]


def pair_kernel(info, state, gains, own, other, bnd_in, bnd, kept, out, w_f, w_g, bbuf, kbuf, sem_f, sem_g, bsem, ksem):
    del bnd_in

    def leave(j):
        layer = LAYERS - 1 - j
        pltpu.make_async_copy(bbuf.at[layer], bnd.at[layer], bsem).start()
        pltpu.make_async_copy(kbuf.at[j], kept.at[j], ksem).start()

    @pl.when(info[0] == 1)
    def _():
        fetch(0, info, own, other, w_f, w_g, sem_f, sem_g)
        fetch(1, info, own, other, w_f, w_g, sem_f, sem_g)

        def step(j, carry):
            y1, y2 = carry
            layer = LAYERS - 1 - j

            @pl.when(j < LAYERS - 2)
            def _():
                fetch(j + 2, info, own, other, w_f, w_g, sem_f, sem_g)

            bbuf[layer, :, 0:CH] = y1.astype(BF16)
            bbuf[layer, :, CH : 2 * CH] = y2.astype(BF16)
            gain_f, gain_g = gain_rows(j, info, gains)
            pre_g = scaled_after(y1, gain_g, arrived(j, own, w_g, sem_g))
            act_g, slope_g = silu_parts(pre_g)
            x2 = y2 - act_g
            pre_f = scaled_after(x2, gain_f, arrived(j, own, w_f, sem_f))
            act_f, slope_f = silu_parts(pre_f)
            x1 = y1 - act_f
            for k, v in enumerate((y1, x2, slope_f, slope_g, pre_f, pre_g)):
                kbuf[j, :, k * CH : (k + 1) * CH] = v

            @pl.when(j > 0)
            def _():
                leave(j - 1)

            return x1, x2

        first = tuple(state[:, k * CH : (k + 1) * CH].astype(F32) for k in range(2))
        last = lax.fori_loop(0, LAYERS, step, first)
        for k in range(2):
            out[:, k * CH : (k + 1) * CH] = last[k].astype(BF16)
        leave(LAYERS - 1)
        pltpu.make_async_copy(bbuf, bnd, bsem).wait()
        pltpu.make_async_copy(kbuf, kept, ksem).wait()


def grad_kernel(info, state, gains, own, other, kept, bnd_in, bnd, out, w_f, w_g, bbuf, kbuf, sem_f, sem_g, bsem, ksem):
    del bnd_in

    @pl.when(info[0] == 1)
    def _():
        pltpu.make_async_copy(kept.at[0], kbuf.at[0], ksem.at[0]).start()
        fetch(0, info, own, other, w_f, w_g, sem_f, sem_g)
        pltpu.make_async_copy(kept.at[1], kbuf.at[1], ksem.at[1]).start()
        fetch(1, info, own, other, w_f, w_g, sem_f, sem_g)

        def step(j, carry):
            gy1, gy2 = carry
            layer = LAYERS - 1 - j
            at = lax.rem(j, 3)

            @pl.when(j < LAYERS - 2)
            def _():
                ahead = lax.rem(j + 2, 3)
                pltpu.make_async_copy(kept.at[j + 2], kbuf.at[ahead], ksem.at[ahead]).start()
                fetch(j + 2, info, own, other, w_f, w_g, sem_f, sem_g)

            bbuf[layer, :, 0:CH] = gy1.astype(BF16)
            bbuf[layer, :, CH : 2 * CH] = gy2.astype(BF16)
            pltpu.make_async_copy(kept.at[0], kbuf.at[at], ksem.at[at]).wait()
            y1, x2, slope_f, slope_g, pre_f, pre_g = (
                kbuf[at, :, k * CH : (k + 1) * CH] for k in range(6)
            )
            gain_f, gain_g = gain_rows(j, info, gains)
            delta_g = (gy2 * slope_g).astype(BF16)
            gz = grad_through(gy1, delta_g, y1, pre_g, arrived(j, own, w_g, sem_g), gain_g)
            pltpu.make_async_copy(bbuf.at[layer], bnd.at[layer], bsem).start()
            delta_f = (gz * slope_f).astype(BF16)
            gx2 = grad_through(gy2, delta_f, x2, pre_f, arrived(j, own, w_f, sem_f), gain_f)
            return gz.astype(BF16).astype(F32), gx2.astype(BF16).astype(F32)

        first = tuple(state[:, k * CH : (k + 1) * CH].astype(F32) for k in range(2))
        last = lax.fori_loop(0, LAYERS, step, first)
        for k in range(2):
            out[:, k * CH : (k + 1) * CH] = last[k].astype(BF16)
        pltpu.make_async_copy(bbuf, bnd, bsem).wait()


BND = jax.ShapeDtypeStruct((LAYERS, ROWS, 2 * CH), BF16)
KEPT = jax.ShapeDtypeStruct((LAYERS, ROWS, 6 * CH), F32)
STATE = jax.ShapeDtypeStruct((ROWS, 2 * CH), BF16)
VMEM = pl.BlockSpec(memory_space=pltpu.VMEM)
HBM = pl.BlockSpec(memory_space=pltpu.HBM)
SMEM = pl.BlockSpec(memory_space=pltpu.SMEM)
WEIGHT_BUFFERS = [
    pltpu.VMEM((3, CH, CH), BF16),
    pltpu.VMEM((3, CH, CH), BF16),
    pltpu.VMEM((LAYERS, ROWS, 2 * CH), BF16),
]
WEIGHT_SEMS = [pltpu.SemaphoreType.DMA((3,)), pltpu.SemaphoreType.DMA((3,)), pltpu.SemaphoreType.DMA]
STAGE_PARAMS = pltpu.CompilerParams(
    vmem_limit_bytes=48 * 2**20
)
STAGE_COST = pl.CostEstimate(
    flops=4 * 8 * ROWS * CH * CH, bytes_accessed=32 * 2**20, transcendentals=0
)


def run_pairs(info, state, gains, own, other, bnd):
    return pl.pallas_call(
        pair_kernel,
        out_shape=(BND, KEPT, STATE),
        in_specs=[SMEM, VMEM, VMEM, HBM, HBM, HBM],
        out_specs=(HBM, HBM, VMEM),
        scratch_shapes=WEIGHT_BUFFERS
        + [pltpu.VMEM(KEPT.shape, F32)]
        + WEIGHT_SEMS
        + [pltpu.SemaphoreType.DMA],
        input_output_aliases={5: 0},
        compiler_params=STAGE_PARAMS,
        cost_estimate=STAGE_COST,
        name="pairs",
    )(info, state, gains, own, other, bnd)


def run_grads(info, state, gains, own, other, kept, bnd):
    return pl.pallas_call(
        grad_kernel,
        out_shape=(BND, STATE),
        in_specs=[SMEM, VMEM, VMEM, HBM, HBM, HBM, HBM],
        out_specs=(HBM, VMEM),
        scratch_shapes=WEIGHT_BUFFERS
        + [pltpu.VMEM((3, ROWS, 6 * CH), F32)]
        + WEIGHT_SEMS
        + [pltpu.SemaphoreType.DMA((3,))],
        input_output_aliases={6: 0},
        compiler_params=STAGE_PARAMS,
        cost_estimate=STAGE_COST,
        name="grads",
    )(info, state, gains, own, other, kept, bnd)


def owner_kernel(info, pb, gb, gains, own, pair, grad, parts, gain_sums, wbuf_f, wbuf_g, sem_f, sem_g):
    rows = pl.ds(info[0] * CH, CH)
    copy_g = pltpu.make_async_copy(own.at[rows, pl.ds(CH, CH)], wbuf_g, sem_g)
    copy_f = pltpu.make_async_copy(own.at[rows, pl.ds(0, CH)], wbuf_f, sem_f)
    copy_g.start()
    copy_f.start()

    def landed(copy, buf):
        copy.wait()
        return buf[...]

    y1, y2 = (pb[:, k * CH : (k + 1) * CH].astype(F32) for k in range(2))
    gy1, gy2 = (gb[:, k * CH : (k + 1) * CH].astype(F32) for k in range(2))
    gain_f, gain_g = gains[0:1, :], gains[1:2, :]
    x1, x2, slope_f, slope_g, inv_f, inv_g, norm_f, norm_g = pair_back(
        y1, y2, lambda: landed(copy_f, wbuf_f), lambda: landed(copy_g, wbuf_g), gain_f, gain_g
    )
    gz, gx2, delta_f, delta_g, back_f, back_g = grad_back(
        gy1,
        gy2,
        y1,
        x2,
        slope_f,
        slope_g,
        inv_f,
        inv_g,
        lambda: wbuf_f[...],
        lambda: wbuf_g[...],
        gain_f,
        gain_g,
    )
    pair[:, 0:CH] = x1
    pair[:, CH : 2 * CH] = x2
    grad[:, 0:CH] = gz.astype(BF16)
    grad[:, CH : 2 * CH] = gx2.astype(BF16)
    gain_sums[0:1, :] = jnp.sum(back_f * x2 * inv_f, axis=0, keepdims=True)
    gain_sums[1:2, :] = jnp.sum(back_g * y1 * inv_g, axis=0, keepdims=True)
    contract = (((0,), (0,)), ((), ()))
    for at, n, d in ((0, norm_f, delta_f), (CH, norm_g, delta_g)):
        for k in range(0, CH, 256):
            part = lax.dot_general(n[:, k : k + 256], d, contract, preferred_element_type=F32)
            for q in range(4):
                yl, z = (k // 64 + q) // 8, (k // 64 + q) % 8
                rows = pl.ds((z * 2 + yl) * 64, 64)
                parts[rows, at : at + CH] = part[q * 64 : (q + 1) * 64].astype(BF16)


def run_owner(info, pb, gb, gains, own):
    vmem = VMEM
    rows = pb.shape[0]
    return pl.pallas_call(
        owner_kernel,
        out_shape=(
            jax.ShapeDtypeStruct((rows, 2 * CH), F32),
            jax.ShapeDtypeStruct((rows, 2 * CH), BF16),
            jax.ShapeDtypeStruct((CH, 2 * CH), BF16),
            jax.ShapeDtypeStruct((2, CH), F32),
        ),
        in_specs=[SMEM, vmem, vmem, vmem, HBM],
        out_specs=(vmem, vmem, vmem, vmem),
        scratch_shapes=[
            pltpu.VMEM((CH, CH), BF16),
            pltpu.VMEM((CH, CH), BF16),
            pltpu.SemaphoreType.DMA,
            pltpu.SemaphoreType.DMA,
        ],
        compiler_params=pltpu.CompilerParams(vmem_limit_bytes=52 * 2**20),
        cost_estimate=pl.CostEstimate(
            flops=12 * rows * CH * CH, bytes_accessed=12 * 2**20, transcendentals=0
        ),
        name="owner",
    )(info, pb, gb, gains, own)


def swapped(array):
    return lax.ppermute(array, "c", [(0, 1), (1, 0)])


def to_owner(bnd):
    mine = lax.all_to_all(bnd, ("yh", "c"), split_axis=0, concat_axis=0, tiled=True)
    return mine.reshape(LAYERS * ROWS, 2 * CH)


def shards(out_pair, out_grad, f_weight, g_weight, gains):
    x, yh, c = (lax.axis_index(a).astype(jnp.int32) for a in ("x", "yh", "c"))
    shard = jnp.concatenate([f_weight[0], g_weight[0]], axis=1)
    own = lax.all_gather(shard, ("yh", "yl", "z"), axis=0, tiled=True)
    near = swapped(gains[0])
    chip_gains = jnp.where(c == 0, jnp.stack([gains[0], near]), jnp.stack([near, gains[0]]))
    far_gains = [
        lax.ppermute(chip_gains, "yh", [(i, (i + by) % 4) for i in range(4)]) for by in (1, 2, 3)
    ]
    all_gains = jnp.stack([chip_gains] + far_gains)
    at = (yh * 2 + c) * ROWS
    pairs = lax.dynamic_slice_in_dim(out_pair, at, ROWS, 0).astype(BF16)
    grads = lax.dynamic_slice_in_dim(out_grad, at, ROWS, 0)
    own, all_gains, pairs, grads = lax.optimization_barrier((own, all_gains, pairs, grads))
    other = swapped(own)
    infos = [jnp.stack([(x == 3 - stage).astype(jnp.int32), c, yh]) for stage in range(4)]
    pb = gb = jnp.zeros(BND.shape, BF16)
    for stage in range(4):
        hop = [(3 - stage, 2 - stage)]
        pb, kept, next_pairs = run_pairs(infos[stage], pairs, all_gains, own, other, pb)
        if stage < 3:
            pairs = lax.ppermute(next_pairs, "x", hop)
            gb, next_grads = run_grads(infos[stage], grads, all_gains, own, other, kept, gb)
            grads = lax.ppermute(next_grads, "x", hop)
            pairs, gb = lax.optimization_barrier((pairs, gb))
    my_pairs = to_owner(pb)
    last = jnp.stack([(x == 0).astype(jnp.int32), c, yh, c + yh])
    gb = run_grads(last, grads, all_gains, own, other, kept, gb)[0]
    my_grads = to_owner(gb)
    pair, grad, parts, gain_part = run_owner(
        jnp.stack([yh, c]), my_pairs, my_grads, gains[0], own
    )
    sums = lax.psum_scatter(parts, "z", scatter_dimension=0, tiled=True)
    gain_total = lax.psum(gain_part, ("yl", "z"))
    sums, gain_total = lax.optimization_barrier((sums, gain_total))
    sums = sums.reshape(2, 64, 2 * CH)
    first = lax.axis_index("yl") == 0
    theirs = lax.ppermute(jnp.where(first, sums[1], sums[0]), "yl", [(0, 1), (1, 0)])
    sums = jnp.where(first, sums[0], sums[1]).astype(F32) + theirs.astype(F32)
    return (pair[None], grad[None], sums[None, :, :CH], sums[None, :, CH:], gain_total[None])


def solution(mesh):
    devices = mesh.devices.reshape(4, 4, 2, 2, 8)
    fine = Mesh(devices, ("x", "yh", "c", "yl", "z"))
    section, dp = ("x", "yh", "c"), ("yl", "z")
    return jax.shard_map(
        shards,
        mesh=fine,
        in_specs=(P(dp, None), P(dp, None), P(section, dp, None), P(section, dp, None), P(section, None, None)),
        out_specs=(
            P(section, dp, None),
            P(section, dp, None),
            P(section, dp, None),
            P(section, dp, None),
            P(section, None, None),
        ),
        check_vma=False,
    )
```
